32 devices in a mesh: gr: 8 (over z, core), gc: 4 (over y, x).
Axes of the slice: x: 2, y: 2, z: 4, core: 2. Of those that a mesh axis runs over, the one named last changes fastest.
Arguments:
- projectors: bfloat16 [2, 8192, 9216], P(None, ('gr', 'gc')), may hold values from -0.0625 to 0.0625
- wavefunctions: bfloat16 [2, 8192, 512], P(None, ('gr', 'gc')), may hold values from -6 to 6
- coupling: float32 [512, 18, 18], P('gc'), may hold values from -1.5 to 1.5
- atom_order: int32 [512], replicated, may hold values from 0 to 511, each once
Outputs:
- coupled: float32 [9216, 512], P('gc', 'gr')
The draws below stay inside these ranges and needn't reach their ends.
Inputs may be any that keep to these rules, and one draw needn't show every extreme that they name: `atom_order`: a permutation of the atoms.
All inputs are finite; a program needn't handle non-finite values.
Results may differ from the reference program's by a relative error of at most 0.0003.
Values sent between devices are 32-bit elements; how exact they have to be, the bound alone decides.
A program may use at most 128 MiB of HBM per device.

```python
import jax
import jax.numpy as jnp
from jax import lax

ATOMS = 512
NH = 18
BANDS = 512
NKB = 9216
NPW = 8192


def spiked(drawn, key, source, target, parts, factor):
    def block_of(position):
        return (jnp.arange(drawn.shape[position]) // (drawn.shape[position] // parts)).reshape((-1,) + (1,) * (drawn.ndim - 1 - position))

    first = jax.random.permutation(key, parts)[block_of(target)]
    second = (block_of(target) + parts // 2) % parts
    return jnp.where((block_of(source) == first) | (block_of(source) == second), factor * drawn, drawn)


def block_scale(own_key, extent, cuts, least, largest):
    level, own = 1.0, jax.random.fold_in(own_key, 6)
    for dim, blocks in cuts:
        heights = jnp.exp(jax.random.uniform(jax.random.fold_in(own, dim), (blocks,), jnp.float32, least / len(cuts), largest / len(cuts)))
        level = level * jnp.repeat(heights, extent[dim] // blocks).reshape([-1 if axis == dim else 1 for axis in range(len(extent))])
    return level


def scatter_about(own_key, shape, width, reach, split=(), dtype=jnp.bfloat16):
    drawn = jax.random.normal(own_key, shape, jnp.float32) * width
    if len(split) > 0:
        drawn = block_scale(own_key, shape, split, -0.22, 0.18) * drawn
    return jnp.clip(drawn, min=-reach, max=reach).astype(dtype)


def heavy_noise(key, extent, width, reach, split, heavy, dtype=jnp.bfloat16):
    drawn = width * jax.random.normal(key, extent, jnp.float32)
    if split:
        drawn = drawn * block_scale(key, extent, split, -0.22, 0.18)
    return jnp.clip(spiked(drawn, jax.random.fold_in(key, 3), *heavy), -reach, reach).astype(dtype)


def setup_inputs(seed: int = 0) -> dict:
    seeds = jax.random.split(jax.random.key(seed), 5)
    return {
        "projectors": heavy_noise(seeds[0], (2, NPW, NKB), (4 * NPW) ** -0.5, 0.0625, ((1, 32),), (1, 2, 32, 2.75)),
        "wavefunctions": scatter_about(seeds[1], (2, NPW, BANDS), 1.0, 6.0, ((1, 32),)),
        "coupling": scatter_about(seeds[2], (ATOMS, NH, NH), NH ** -0.5, 1.5, ((0, 4),), jnp.float32),
        "atom_order": jax.random.permutation(seeds[3], ATOMS).astype(jnp.int32),
    }


def reference(projectors, wavefunctions, coupling, atom_order):
    shaped = projectors.reshape(2, NPW, ATOMS, NH)
    waves = wavefunctions.reshape(2 * NPW, BANDS)
    blocks = atom_order.reshape(-1, 32)

    def one_block(picked_ids):
        columns = jnp.take(shaped, picked_ids, axis=2).reshape(2 * NPW, 32 * NH)
        term = lax.dot_general(columns, waves, (((0,), (0,)), ((), ())), preferred_element_type=jnp.float32)
        return 2.0 * term

    becp = lax.map(one_block, blocks).reshape(ATOMS, NH, BANDS)
    coupled = jnp.einsum("kij,kjb->kib", coupling.astype(jnp.float32), becp, precision=lax.Precision.HIGHEST)
    return coupled.reshape(NKB, BANDS)
```

```python
import functools
import math

import jax
import jax.numpy as jnp
from jax import lax
from jax.experimental import pallas as pl
from jax.experimental.pallas import tpu as pltpu
from jax.sharding import PartitionSpec as P

MESH = pl.DeviceIdType.MESH
GROUP = 8
GROUPS = 8
LANES = 128
STRIP = 1152
BATCHES = ((0, 1, 2, 3), (4, 5, 6, 7), (0, 1, 2, 3), (4, 5, 6, 7))
FIRST_PASS = 2
PACKS = 4
RESULTS = 4
MULTIPLY, COUPLINGS = -1, -2

UNITS = (
    (0, 0, "ABZ"), (1, 0, "ZBA"), (2, 0, "BAZ"), (3, 0, "ZAB"),
    (4, 0, "ABZ"), (5, 0, "ZAB"), (6, 0, "ZBA"), (7, 0, "ZBA"),
    (0, 1, "BAZ"), (1, 1, "ABZ"), (2, 1, "BAZ"), (3, 1, "ABZ"),
    (4, 1, "BAZ"), (5, 1, "ABZ"), (6, 1, "BAZ"), (7, 1, "ABZ"),
)
SPLIT = (0, 1, 2)
ORDER = (
    -1, -1, 0, 1, 2, 128, 7, 129, 130, 16, 17, 18, 3, -1, -1, 11, 8, 6, 27, 19, 112, 4, 13, 10, 24, 32, 15, 113, -2,
    33, 29, 114, 22, 23, 43, 12, 31, 26, 35, 9, 45, 49, 20, 5, 38, 21, 14, 40, 47, 30, 48, 51, 39, 37, 61, 54, 59,
    25, 63, 75, 56, 42, 28, 36, 77, 64, 55, 46, 53, 41, 58, 34, 72, 74, 44, 67, 80, 62, 70, 71, 79, 78, 52, 50, 95,
    57, 69, 93, 86, 68, 65, 91, 90, 96, 60, 66, 83, 87, 85, 73, 84, 107, 111, 109, 88, 81, 100, 82, 102, 106, 99,
    76, 103, 94, 98, 101, 89, 92, 110, 108, 104, 105, 97,
)


def receiving():
    found, count = {}, 0
    for u, (_, h, path) in enumerate(UNITS):
        at_z = path.index("Z")
        if at_z == 0:
            sets = [(0,), (3, 6), (4, 1), (2,)]
        elif at_z == 1:
            sets = [(0,), (1,), (3, 6), (4, 2)]
        else:
            sets = [(0,), (1,), (2,), (3, 6), (4,)] + ([(5,)] if h == 1 else [])
        if u in SPLIT:
            sets.append((7,))
        for slots in sets:
            found.update({(u, slot): count for slot in slots})
            count += 1
    return found, count


RECEIVING, RECEIVES = receiving()


def plain(projectors, wavefunctions, coupling, atom_order):
    rows_here, nkb = projectors.shape[1:]
    bands = wavefunctions.shape[2]
    atoms = atom_order.shape[0]
    nh = nkb // atoms
    shaped = projectors.reshape(2, rows_here, atoms, nh)
    waves = wavefunctions.reshape(2 * rows_here, bands)
    columns = jnp.take(shaped, atom_order, axis=2).reshape(2 * rows_here, nkb)
    term = lax.dot_general(columns, waves, (((0,), (0,)), ((), ())), preferred_element_type=jnp.float32)
    partial_rows = lax.psum_scatter(2.0 * term, "gc", scatter_dimension=0, tiled=True)
    becp = lax.psum_scatter(partial_rows, "gr", scatter_dimension=1, tiled=True)
    local_atoms = coupling.shape[0]
    becp = becp.reshape(local_atoms, nh, becp.shape[1])
    coupled = jnp.einsum("kij,kjb->kib", coupling, becp, precision=lax.Precision.HIGHEST)
    return coupled.reshape(local_atoms * nh, becp.shape[2])


def kernel(
    size, nh, apo, order_in, proj_ref, wave_in, coup_in, out_ref, order_ref, turned, fin, mats, nat, strip, wave, coup,
    oth, rec, strip_sem, load_sem, send_sem, recv_sem, fin_send, fin_recv, out_sem,
):
    gr, gc = lax.axis_index("gr"), lax.axis_index("gc")
    core, z = lax.rem(gr, 2), gr // 2
    me = {"A": gc // size["B"], "B": lax.rem(gc, size["B"])}
    half = apo // 2
    rows = GROUP * nh
    side = z // 2
    near, far = side, 1 - side
    way = 1 - 2 * side
    end = (z == 0) | (z == size["Z"] - 1)
    middle = jnp.logical_not(end)

    def at(a, b, zz):
        return {"gr": zz * 2 + core, "gc": a * size["B"] + b}

    partner = {"gr": gr + 1 - 2 * core, "gc": gc}
    other = {"A": at(1 - me["A"], me["B"], z), "B": at(me["A"], 1 - me["B"], z)}
    inward = at(me["A"], me["B"], z + way)
    outward = at(me["A"], me["B"], lax.rem(z - way + size["Z"], size["Z"]))

    strips = proj_ref.shape[1] // STRIP

    def load(number):
        return pltpu.make_async_copy(proj_ref.at[:, pl.ds(number * STRIP, STRIP)], strip.at[number], strip_sem.at[number])

    wave_loads = [
        pltpu.make_async_copy(wave_in.at[:, pl.ds(zz * LANES, LANES)], wave.at[:, pl.ds(i * LANES, LANES)], load_sem.at[i])
        for i, zz in enumerate((0, 3, 1, 2))
    ]
    coup_load = pltpu.make_async_copy(coup_in, coup, load_sem.at[4])
    order_load = pltpu.make_async_copy(order_in, order_ref, load_sem.at[5])
    wave_loads[0].start()
    wave_loads[1].start()
    for number in range(strips):
        load(number).start()
    order_load.start()
    wave_loads[2].start()
    wave_loads[3].start()
    coup_load.start()

    greeted = [partner, other["A"], other["B"], inward, outward]
    barrier = pltpu.get_barrier_semaphore()
    for device in greeted:
        pl.semaphore_signal(barrier, inc=1, device_id=device, device_id_type=MESH)

    def multiply(batch):
        h = int(batch >= FIRST_PASS)
        if batch in (0, FIRST_PASS):
            wave_loads[2 * h].wait()
            wave_loads[2 * h + 1].wait()
        if h == 0:
            for number in BATCHES[batch]:
                load(number).wait()
        for number in BATCHES[batch]:
            term = lax.dot_general(
                strip[number], wave[:, 2 * h * LANES:2 * (h + 1) * LANES],
                (((0,), (0,)), ((), ())), preferred_element_type=jnp.float32,
            )
            for i in range(2):
                nat[2 * h + i, pl.ds(number * STRIP, STRIP), :] = term[:, i * LANES:(i + 1) * LANES]

    def first_of(u):
        path = UNITS[u][2]
        return far if path[0] == "Z" else 1 - me[path[0]]

    def gather(u, which, store, fixed=None):
        g, h, path = UNITS[u]

        def body(t, carry):
            of = {}
            if fixed is None or path[0] == "Z":
                of = {"A": t // size["B"], "B": lax.rem(t, size["B"])}
            else:
                of = {path[0]: fixed, "B" if path[0] == "A" else "A": t}
            owner = of["A"] * size["B"] + of["B"]
            for i in range(GROUP):
                row = order_ref[owner * apo + which * half + g * GROUP + i] * nh
                for zi in ((0, 1) if fixed is None or path[0] != "Z" else (fixed,)):
                    of["Z"] = zi
                    where = tuple(of[d] for d in path) + (pl.ds(i * nh, nh), slice(None))
                    store(where, nat[2 * h + zi, pl.ds(row, nh), :])
            return carry

        lax.fori_loop(0, size["A"] * size["B"] if fixed is None or path[0] == "Z" else 2, body, 0)

    def add(dst, prefix, src):
        rest = src.shape[:-2]
        if len(rest) == 2:
            def body(t, carry):
                where = (t // rest[1], lax.rem(t, rest[1]))
                dst[tuple(prefix) + where] = dst[tuple(prefix) + where] + src[where]
                return carry

            lax.fori_loop(0, math.prod(rest), body, 0)
        elif rest:
            for t in range(rest[0]):
                dst[tuple(prefix) + (t,)] = dst[tuple(prefix) + (t,)] + src[t]
        else:
            dst[tuple(prefix)] = dst[tuple(prefix)] + src[...]

    def copy(u, slot, src, dst, device):
        return pltpu.make_async_remote_copy(
            src_ref=src, dst_ref=dst, send_sem=send_sem.at[sending(u, slot)], recv_sem=recv_sem.at[RECEIVING[u, slot]],
            device_id=device, device_id_type=MESH,
        )

    def sending(u, slot):
        if slot == 0:
            return len(UNITS) + packs.index(u) % PACKS
        if slot == 7:
            return len(UNITS) + PACKS + SPLIT.index(u)
        if slot == 5:
            return len(UNITS) + PACKS + len(SPLIT) + UNITS[u][0]
        return u

    def packed(u):
        return oth.at[packs.index(u) % PACKS]

    def head(u, rest):
        if u not in SPLIT:
            return ()
        return (1 - first_of(u) if rest else first_of(u),)

    def buffers(u, slot):
        if slot in (0, 7):
            return rec[u][0].at[head(u, slot == 7)] if u in SPLIT else rec[u][0]
        return rec[u][slot]

    def send(u, slot):
        g, h, path = UNITS[u]
        d1, d2 = [d for d in path if d != "Z"]
        me1, me2 = me[d1], me[d2]
        to = buffers(u, slot)
        if slot in (0, 7):
            return copy(u, slot, packed(u).at[head(u, slot == 7)] if u in SPLIT else packed(u), to, partner)
        at_z = path.index("Z")
        place = (me1, me2)[:at_z]
        src = {3: place + (far,), 4: place + (far,), 5: place + (near,), 6: place + (near,)}
        if at_z == 0:
            src[1], src[2] = (near, 1 - me1), (near, me1, 1 - me2)
        elif at_z == 1:
            src[1], src[2] = (1 - me1,), (me1, near, 1 - me2)
        else:
            src[1], src[2] = (1 - me1,), (me1, 1 - me2)
        device = {1: other[d1], 2: other[d2], 3: inward, 4: inward, 5: inward, 6: outward}[slot]
        return copy(u, slot, rec[u][0].at[src[slot]], to, device)

    def arrived(u, slot):
        to = buffers(u, slot)
        copy(u, slot, to, to, partner).wait_recv()

    def fin_copy(g, turn):
        part = fin.at[core, pl.ds(g * rows, rows)]
        return pltpu.make_async_remote_copy(
            src_ref=part, dst_ref=part, send_sem=fin_send.at[turn % 2], recv_sem=fin_recv.at[g],
            device_id=partner, device_id_type=MESH,
        )

    def ready(groups):
        return {t for t in range(blocks) if all(g in groups for g in range(t * LANES // rows, (t * LANES + LANES - 1) // rows + 1))}

    def result(t, mine, turn):
        which = core if mine else 1 - core
        columns = pl.ds(pl.multiple_of((which * blocks + t) * LANES, LANES), LANES)
        return pltpu.make_async_copy(turned.at[:, columns], out_ref.at[:, columns], out_sem.at[turn % RESULTS])

    def turn(t, mine):
        which = core if mine else 1 - core
        block = fin[which, pl.ds(t * LANES, LANES), :].T
        own = LANES // 2
        to = pl.ds(pl.multiple_of((which * blocks + t) * LANES, LANES), LANES)
        turned[:, to] = jnp.where(core == 0, block[:own], block[own:])

    def come(g):
        part = fin.at[1 - core, pl.ds(g * rows, rows)]
        pltpu.make_async_remote_copy(
            src_ref=part, dst_ref=part, send_sem=fin_send.at[0], recv_sem=fin_recv.at[g],
            device_id=partner, device_id_type=MESH,
        ).wait_recv()

    def fetch(role, groups):
        came = state[role][1]
        for g in groups:
            if g not in came:
                come(g)
                came.append(g)

    def turns(role):
        made, came, mine, theirs = state[role]
        found = [(t, True) for t in sorted(ready(made) - mine)] + [(t, False) for t in sorted(ready(came) - theirs)]
        for t, own in found:
            turn(t, own)
            (mine if own else theirs).add(t)
        return found

    def put(role, found):
        given = results[role]
        for t, own in found:
            if len(given) >= RESULTS:
                result(*given[-RESULTS], len(given) - RESULTS).wait()
            result(t, own, len(given)).start()
            given.append((t, own))

    def final(u, own, others, role):
        g = UNITS[u][0]
        made = state[role][0]
        fetch(role, made[:-1])
        found = turns(role)
        for i in range(GROUP):
            here = (pl.ds(i * nh, nh), slice(None))
            becp = rec[u][0][own + here]
            for slot in others:
                becp = becp + rec[u][slot][here]
            fin[core, pl.ds((g * GROUP + i) * nh, nh), :] = jnp.dot(
                mats[:, pl.ds(core * half + g * GROUP + i, 1), :].reshape(nh, nh), 2.0 * becp,
                precision=lax.Precision.HIGHEST, preferred_element_type=jnp.float32,
            )
        if len(made) >= 2:
            fin_copy(made[-2], len(made) - 2).wait_send()
        fin_copy(g, len(made)).start()
        made.append(g)
        put(role, found)
        if len(made) == GROUPS:
            put(role, turns(role))
            fetch(role, made)
            put(role, turns(role))

    blocks = GROUPS * rows // LANES
    state = {role: ([], [], set(), set()) for role in ("end", "middle")}
    results = {"end": [], "middle": []}
    packs = [code % 16 for code in ORDER if 0 <= code < 16]
    pending = {"end": {}, "middle": {}}

    def start(u, slot, role):
        roles = ("end", "middle") if role == "all" else (role,)
        key = sending(u, slot)
        before = {pending[r].get(key) for r in roles}
        assert len(before) == 1
        for old in before:
            if old is not None:
                send(*old).wait_send()
        send(u, slot).start()
        for r in roles:
            pending[r][key] = (u, slot)

    def finish(role):
        for u, slot in pending[role].values():
            send(u, slot).wait_send()
        made, given = state[role][0], results[role]
        for turn in range(len(made) - 2, len(made)):
            fin_copy(made[turn], turn).wait_send()
        for turn in range(len(given) - RESULTS, len(given)):
            result(*given[turn], turn).wait()

    def relay(u, slot, place, out):
        @pl.when(middle)
        def _():
            arrived(u, slot)
            add(rec[u][0], place, rec[u][slot])
            start(u, out, "middle")

    def phase(p, u):
        g, h, path = UNITS[u]
        d1, d2 = [d for d in path if d != "Z"]
        me1, me2 = me[d1], me[d2]
        at_z = path.index("Z")
        if p in (0, 8):
            place = packs.index(u)
            target = packed(u)

            def keep(where, value):
                target[where] = value

            if p == 0 and place >= PACKS:
                before = packs[place - PACKS]
                for slot in (0, 7) if before in SPLIT else (0,):
                    send(before, slot).wait_send()
                    for r in ("end", "middle"):
                        del pending[r][sending(before, slot)]
            gather(u, 1 - core, keep, *head(u, p == 8))
            start(u, 7 if p == 8 else 0, "all")
            return
        if p in (1, 7):
            arrived(u, 0 if p == 1 else 7)
            both = rec[u][0]

            def total(where, value):
                both[where] = both[where] + value

            gather(u, core, total, *head(u, p == 7))
            if p == 7:
                return
        if at_z == 2:
            if p == 1:
                start(u, 1, "all")
            elif p == 2:
                arrived(u, 1)
                add(rec[u][0], (me1,), rec[u][1])
                start(u, 2, "all")
            elif p == 3:
                arrived(u, 2)
                add(rec[u][0], (me1, me2), rec[u][2])

                @pl.when(end)
                def _():
                    start(u, 3, "end")
                    if h == 1:
                        start(u, 5, "end")
            elif p == 4:
                relay(u, 3, (me1, me2, far), 4)
            elif p == 5 and h == 0:
                relay(u, 4, (me1, me2, near), 6)
            elif p == 5:
                @pl.when(middle)
                def _():
                    arrived(u, 5)
                    arrived(u, 4)
                    final(u, (me1, me2, near), (5, 4), "middle")
            elif h == 0:
                @pl.when(end)
                def _():
                    arrived(u, 6)
                    final(u, (me1, me2, near), (6,), "end")
        elif at_z == 1:
            if p == 1:
                start(u, 1, "all")
            elif p == 2:
                arrived(u, 1)
                add(rec[u][0], (me1,), rec[u][1])

                @pl.when(end)
                def _():
                    start(u, 3, "end")
            elif p == 3:
                relay(u, 3, (me1, far), 4)
            elif p == 4:
                relay(u, 4, (me1, near), 6)
            elif p == 5:
                @pl.when(end)
                def _():
                    arrived(u, 6)
                    add(rec[u][0], (me1, near), rec[u][6])
                    start(u, 2, "end")
            else:
                @pl.when(end)
                def _():
                    arrived(u, 2)
                    final(u, (me1, near, me2), (2,), "end")
        else:
            if p == 1:
                @pl.when(end)
                def _():
                    start(u, 3, "end")
            elif p == 2:
                relay(u, 3, (far,), 4)
            elif p == 3:
                relay(u, 4, (near,), 6)
            elif p == 4:
                @pl.when(end)
                def _():
                    arrived(u, 6)
                    add(rec[u][0], (near,), rec[u][6])
                    start(u, 1, "end")
            elif p == 5:
                @pl.when(end)
                def _():
                    arrived(u, 1)
                    add(rec[u][0], (near, me1), rec[u][1])
                    start(u, 2, "end")
            else:
                @pl.when(end)
                def _():
                    arrived(u, 2)
                    final(u, (near, me1, me2), (2,), "end")

    multiplied, greeting = 0, True
    for code in ORDER:
        if code == MULTIPLY:
            multiply(multiplied)
            multiplied += 1
        elif code == COUPLINGS:
            coup_load.wait()
            for i in range(nh):
                mats[i] = coup[i].T
        else:
            if greeting:
                pl.semaphore_wait(barrier, len(greeted))
                order_load.wait()
                greeting = False
            phase(code // 16, code % 16)

    @pl.when(end)
    def _():
        finish("end")

    @pl.when(middle)
    def _():
        finish("middle")


def routed(size, projectors, wavefunctions, coupling, atom_order):
    rows_here, nkb = projectors.shape[1:]
    bands = wavefunctions.shape[2]
    atoms = atom_order.shape[0]
    nh, apo = nkb // atoms, coupling.shape[0]
    tile = (GROUP * nh, LANES)
    f32 = jnp.float32
    rec = []
    for _, h, path in UNITS:
        if path[0] == "Z":
            shapes = {0: (2, 2, 2), 1: (2,), 2: (), 3: (2, 2), 4: (2, 2), 6: (2, 2)}
        elif path[1] == "Z":
            shapes = {0: (2, 2, 2), 1: (2, 2), 2: (), 3: (2,), 4: (2,), 6: (2,)}
        else:
            shapes = {0: (2, 2, 2), 1: (2, 2), 2: (2,), 3: (), 4: ()}
            shapes[6 if h == 0 else 5] = ()
        rec.append({slot: pltpu.VMEM(shape + tile, f32) for slot, shape in shapes.items()})
    out = pl.pallas_call(
        functools.partial(kernel, size, nh, apo),
        out_shape=jax.ShapeDtypeStruct((LANES // 2, apo * nh), f32),
        in_specs=[
            pl.BlockSpec(memory_space=pl.ANY),
            pl.BlockSpec(memory_space=pl.ANY),
            pl.BlockSpec(memory_space=pl.ANY),
            pl.BlockSpec(memory_space=pl.ANY),
        ],
        out_specs=pl.BlockSpec(memory_space=pl.ANY),
        scratch_shapes=[
            pltpu.SMEM((atoms,), jnp.int32),
            pltpu.VMEM((LANES // 2, apo * nh), f32),
            pltpu.VMEM((2, apo * nh // 2, LANES), f32),
            pltpu.VMEM((nh, apo, nh), f32),
            pltpu.VMEM((size["Z"], nkb, LANES), f32),
            pltpu.VMEM((nkb // STRIP, 2 * rows_here, STRIP), projectors.dtype),
            pltpu.VMEM((2 * rows_here, bands), wavefunctions.dtype),
            pltpu.VMEM((nh, nh, apo), f32),
            pltpu.VMEM((PACKS, 2, 2, 2) + tile, f32),
            rec,
            pltpu.SemaphoreType.DMA((nkb // STRIP,)),
            pltpu.SemaphoreType.DMA((6,)),
            pltpu.SemaphoreType.DMA((len(UNITS) + PACKS + len(SPLIT) + GROUPS,)),
            pltpu.SemaphoreType.DMA((RECEIVES,)),
            pltpu.SemaphoreType.DMA((2,)),
            pltpu.SemaphoreType.DMA((GROUPS,)),
            pltpu.SemaphoreType.DMA((RESULTS,)),
        ],
        compiler_params=pltpu.CompilerParams(
            collective_id=0, has_side_effects=True, vmem_limit_bytes=67_043_328
        ),
    )(
        atom_order, projectors.reshape(2 * rows_here, nkb), wavefunctions.reshape(2 * rows_here, bands),
        jnp.transpose(coupling, (1, 2, 0)),
    )
    return out.T


def solution(mesh):
    gr, gc = mesh.shape["gr"], mesh.shape["gc"]
    wide = max(d for d in range(1, math.isqrt(gc) + 1) if gc % d == 0)
    size = {"A": wide, "B": gc // wide, "Z": gr // 2}

    def shards(projectors, wavefunctions, coupling, atom_order):
        fits = (
            gr % 2 == 0
            and size == {"A": 2, "B": 2, "Z": 4}
            and wavefunctions.shape[2] == size["Z"] * LANES
            and coupling.shape[0] == 2 * GROUP * GROUPS
            and coupling.shape[0] == LANES
            and projectors.shape[2] == sum(len(b) for b in BATCHES) // 2 * STRIP
        )
        if fits:
            return routed(size, projectors, wavefunctions, coupling, atom_order)
        return plain(projectors, wavefunctions, coupling, atom_order)

    return jax.shard_map(
        shards,
        mesh=mesh,
        in_specs=(
            P(None, ("gr", "gc"), None),
            P(None, ("gr", "gc"), None),
            P("gc", None, None),
            P(),
        ),
        out_specs=P("gc", "gr"),
        check_vma=False,
    )
```

```python
import functools
import math

import jax
import jax.numpy as jnp
from jax import lax
from jax.experimental import pallas as pl
from jax.experimental.pallas import tpu as pltpu
from jax.sharding import PartitionSpec as P

MESH = pl.DeviceIdType.MESH
GROUP = 8
GROUPS = 8
LANES = 128
STRIP = 1152
BATCHES = ((0, 1), (2, 3), (4, 5), (6, 7), (0, 1, 2, 3), (4, 5, 6, 7))
FIRST_PASS = 4
PACKS = 4
RESULTS = 4
MULTIPLY, COUPLINGS = -1, -2

UNITS = (
    (0, 0, "ZAB"), (1, 0, "ABZ"), (2, 0, "BAZ"), (3, 0, "ZBA"),
    (4, 0, "ABZ"), (5, 0, "ZAB"), (6, 0, "ZBA"), (7, 0, "ZBA"),
    (0, 1, "BAZ"), (1, 1, "ABZ"), (2, 1, "BAZ"), (3, 1, "ABZ"),
    (4, 1, "BAZ"), (5, 1, "ABZ"), (6, 1, "BAZ"), (7, 1, "ABZ"),
)
SPLIT = (0, 1, 2)
ORDER = (
    -1, -1, -1, -1, 1, 2, 7, 130, 129, 17, 18, 23, -1, 4, -1, 10, 0, 20, 114, 26, 11, 128, 16, 27, 113, 39, 15, 31,
    112, 3, -2, 32, 19, 14, 33, 42, 6, 36, 55, 30, 22, 13, 29, 12, 35, 28, 52, 48, 38, 51, 47, 34, 43, 68, 49, 5,
    21, 54, 58, 44, 9, 37, 25, 45, 8, 24, 63, 74, 46, 84, 50, 53, 66, 60, 71, 64, 79, 59, 65, 75, 41, 95, 40, 67,
    61, 70, 62, 77, 76, 81, 57, 69, 78, 87, 90, 56, 100, 93, 82, 106, 83, 73, 97, 80, 85, 86, 103, 94, 72, 96, 89,
    92, 111, 110, 105, 99, 98, 101, 102, 91, 88, 107, 108, 109, 104,
)


def receiving():
    found, count = {}, 0
    for u, (_, h, path) in enumerate(UNITS):
        at_z = path.index("Z")
        if at_z == 0:
            sets = [(0,), (3, 6), (4, 1), (2,)]
        elif at_z == 1:
            sets = [(0,), (1,), (3, 6), (4, 2)]
        else:
            sets = [(0,), (1,), (2,), (3, 6), (4,)] + ([(5,)] if h == 1 else [])
        if u in SPLIT:
            sets.append((7,))
        for slots in sets:
            found.update({(u, slot): count for slot in slots})
            count += 1
    return found, count


RECEIVING, RECEIVES = receiving()


def plain(projectors, wavefunctions, coupling, atom_order):
    rows_here, nkb = projectors.shape[1:]
    bands = wavefunctions.shape[2]
    atoms = atom_order.shape[0]
    nh = nkb // atoms
    shaped = projectors.reshape(2, rows_here, atoms, nh)
    waves = wavefunctions.reshape(2 * rows_here, bands)
    columns = jnp.take(shaped, atom_order, axis=2).reshape(2 * rows_here, nkb)
    term = lax.dot_general(columns, waves, (((0,), (0,)), ((), ())), preferred_element_type=jnp.float32)
    partial_rows = lax.psum_scatter(2.0 * term, "gc", scatter_dimension=0, tiled=True)
    becp = lax.psum_scatter(partial_rows, "gr", scatter_dimension=1, tiled=True)
    local_atoms = coupling.shape[0]
    becp = becp.reshape(local_atoms, nh, becp.shape[1])
    coupled = jnp.einsum("kij,kjb->kib", coupling, becp, precision=lax.Precision.HIGHEST)
    return coupled.reshape(local_atoms * nh, becp.shape[2])


def kernel(
    size, nh, apo, order_in, proj_ref, wave_in, coup_in, out_ref, order_ref, turned, fin, mats, nat, strip, wave, coup,
    oth, rec, strip_sem, load_sem, send_sem, recv_sem, fin_send, fin_recv, out_sem,
):
    gr, gc = lax.axis_index("gr"), lax.axis_index("gc")
    core, z = lax.rem(gr, 2), gr // 2
    me = {"A": gc // size["B"], "B": lax.rem(gc, size["B"])}
    half = apo // 2
    rows = GROUP * nh
    side = z // 2
    near, far = side, 1 - side
    way = 1 - 2 * side
    end = (z == 0) | (z == size["Z"] - 1)
    middle = jnp.logical_not(end)

    def at(a, b, zz):
        return {"gr": zz * 2 + core, "gc": a * size["B"] + b}

    partner = {"gr": gr + 1 - 2 * core, "gc": gc}
    other = {"A": at(1 - me["A"], me["B"], z), "B": at(me["A"], 1 - me["B"], z)}
    inward = at(me["A"], me["B"], z + way)
    outward = at(me["A"], me["B"], lax.rem(z - way + size["Z"], size["Z"]))

    strips = proj_ref.shape[1] // STRIP

    def load(number):
        return pltpu.make_async_copy(proj_ref.at[:, pl.ds(number * STRIP, STRIP)], strip.at[number], strip_sem.at[number])

    wave_loads = [
        pltpu.make_async_copy(wave_in.at[:, pl.ds(zz * LANES, LANES)], wave.at[:, pl.ds(i * LANES, LANES)], load_sem.at[i])
        for i, zz in enumerate((0, 3, 1, 2))
    ]
    coup_load = pltpu.make_async_copy(coup_in, coup, load_sem.at[4])
    order_load = pltpu.make_async_copy(order_in, order_ref, load_sem.at[5])
    wave_loads[0].start()
    wave_loads[1].start()
    for number in range(strips):
        load(number).start()
    order_load.start()
    wave_loads[2].start()
    wave_loads[3].start()
    coup_load.start()

    greeted = [partner, other["A"], other["B"], inward, outward]
    barrier = pltpu.get_barrier_semaphore()
    for device in greeted:
        pl.semaphore_signal(barrier, inc=1, device_id=device, device_id_type=MESH)

    def multiply(batch):
        h = int(batch >= FIRST_PASS)
        if batch in (0, FIRST_PASS):
            wave_loads[2 * h].wait()
            wave_loads[2 * h + 1].wait()
        if h == 0:
            for number in BATCHES[batch]:
                load(number).wait()
        for number in BATCHES[batch]:
            term = lax.dot_general(
                strip[number], wave[:, 2 * h * LANES:2 * (h + 1) * LANES],
                (((0,), (0,)), ((), ())), preferred_element_type=jnp.float32,
            )
            for i in range(2):
                nat[2 * h + i, pl.ds(number * STRIP, STRIP), :] = term[:, i * LANES:(i + 1) * LANES]

    def first_of(u):
        path = UNITS[u][2]
        return far if path[0] == "Z" else 1 - me[path[0]]

    def gather(u, which, store, fixed=None):
        g, h, path = UNITS[u]

        def body(t, carry):
            of = {}
            if fixed is None or path[0] == "Z":
                of = {"A": t // size["B"], "B": lax.rem(t, size["B"])}
            else:
                of = {path[0]: fixed, "B" if path[0] == "A" else "A": t}
            owner = of["A"] * size["B"] + of["B"]
            for i in range(GROUP):
                row = order_ref[owner * apo + which * half + g * GROUP + i] * nh
                for zi in ((0, 1) if fixed is None or path[0] != "Z" else (fixed,)):
                    of["Z"] = zi
                    where = tuple(of[d] for d in path) + (pl.ds(i * nh, nh), slice(None))
                    store(where, nat[2 * h + zi, pl.ds(row, nh), :])
            return carry

        lax.fori_loop(0, size["A"] * size["B"] if fixed is None or path[0] == "Z" else 2, body, 0)

    def add(dst, prefix, src):
        rest = src.shape[:-2]
        if len(rest) == 2:
            def body(t, carry):
                where = (t // rest[1], lax.rem(t, rest[1]))
                dst[tuple(prefix) + where] = dst[tuple(prefix) + where] + src[where]
                return carry

            lax.fori_loop(0, math.prod(rest), body, 0)
        elif rest:
            for t in range(rest[0]):
                dst[tuple(prefix) + (t,)] = dst[tuple(prefix) + (t,)] + src[t]
        else:
            dst[tuple(prefix)] = dst[tuple(prefix)] + src[...]

    def copy(u, slot, src, dst, device):
        return pltpu.make_async_remote_copy(
            src_ref=src, dst_ref=dst, send_sem=send_sem.at[sending(u, slot)], recv_sem=recv_sem.at[RECEIVING[u, slot]],
            device_id=device, device_id_type=MESH,
        )

    def sending(u, slot):
        if slot == 0:
            return len(UNITS) + packs.index(u) % PACKS
        if slot == 7:
            return len(UNITS) + PACKS + SPLIT.index(u)
        if slot == 5:
            return len(UNITS) + PACKS + len(SPLIT) + UNITS[u][0]
        return u

    def packed(u):
        return oth.at[packs.index(u) % PACKS]

    def head(u, rest):
        if u not in SPLIT:
            return ()
        return (1 - first_of(u) if rest else first_of(u),)

    def buffers(u, slot):
        if slot in (0, 7):
            return rec[u][0].at[head(u, slot == 7)] if u in SPLIT else rec[u][0]
        return rec[u][slot]

    def send(u, slot):
        g, h, path = UNITS[u]
        d1, d2 = [d for d in path if d != "Z"]
        me1, me2 = me[d1], me[d2]
        to = buffers(u, slot)
        if slot in (0, 7):
            return copy(u, slot, packed(u).at[head(u, slot == 7)] if u in SPLIT else packed(u), to, partner)
        at_z = path.index("Z")
        place = (me1, me2)[:at_z]
        src = {3: place + (far,), 4: place + (far,), 5: place + (near,), 6: place + (near,)}
        if at_z == 0:
            src[1], src[2] = (near, 1 - me1), (near, me1, 1 - me2)
        elif at_z == 1:
            src[1], src[2] = (1 - me1,), (me1, near, 1 - me2)
        else:
            src[1], src[2] = (1 - me1,), (me1, 1 - me2)
        device = {1: other[d1], 2: other[d2], 3: inward, 4: inward, 5: inward, 6: outward}[slot]
        return copy(u, slot, rec[u][0].at[src[slot]], to, device)

    def arrived(u, slot):
        to = buffers(u, slot)
        copy(u, slot, to, to, partner).wait_recv()

    def fin_copy(g, turn):
        part = fin.at[core, pl.ds(g * rows, rows)]
        return pltpu.make_async_remote_copy(
            src_ref=part, dst_ref=part, send_sem=fin_send.at[turn % 2], recv_sem=fin_recv.at[g],
            device_id=partner, device_id_type=MESH,
        )

    def ready(groups):
        return {t for t in range(blocks) if all(g in groups for g in range(t * LANES // rows, (t * LANES + LANES - 1) // rows + 1))}

    def result(t, mine, turn):
        which = core if mine else 1 - core
        columns = pl.ds(pl.multiple_of((which * blocks + t) * LANES, LANES), LANES)
        return pltpu.make_async_copy(turned.at[:, columns], out_ref.at[:, columns], out_sem.at[turn % RESULTS])

    def turn(t, mine):
        which = core if mine else 1 - core
        block = fin[which, pl.ds(t * LANES, LANES), :].T
        own = LANES // 2
        to = pl.ds(pl.multiple_of((which * blocks + t) * LANES, LANES), LANES)
        turned[:, to] = jnp.where(core == 0, block[:own], block[own:])

    def come(g):
        part = fin.at[1 - core, pl.ds(g * rows, rows)]
        pltpu.make_async_remote_copy(
            src_ref=part, dst_ref=part, send_sem=fin_send.at[0], recv_sem=fin_recv.at[g],
            device_id=partner, device_id_type=MESH,
        ).wait_recv()

    def fetch(role, groups):
        came = state[role][1]
        for g in groups:
            if g not in came:
                come(g)
                came.append(g)

    def turns(role):
        made, came, mine, theirs = state[role]
        found = [(t, True) for t in sorted(ready(made) - mine)] + [(t, False) for t in sorted(ready(came) - theirs)]
        for t, own in found:
            turn(t, own)
            (mine if own else theirs).add(t)
        return found

    def put(role, found):
        given = results[role]
        for t, own in found:
            if len(given) >= RESULTS:
                result(*given[-RESULTS], len(given) - RESULTS).wait()
            result(t, own, len(given)).start()
            given.append((t, own))

    def final(u, own, others, role):
        g = UNITS[u][0]
        made = state[role][0]
        fetch(role, made[:-1])
        found = turns(role)
        for i in range(GROUP):
            here = (pl.ds(i * nh, nh), slice(None))
            becp = rec[u][0][own + here]
            for slot in others:
                becp = becp + rec[u][slot][here]
            fin[core, pl.ds((g * GROUP + i) * nh, nh), :] = jnp.dot(
                mats[:, pl.ds(core * half + g * GROUP + i, 1), :].reshape(nh, nh), 2.0 * becp,
                precision=lax.Precision.HIGHEST, preferred_element_type=jnp.float32,
            )
        if len(made) >= 2:
            fin_copy(made[-2], len(made) - 2).wait_send()
        fin_copy(g, len(made)).start()
        made.append(g)
        put(role, found)
        if len(made) == GROUPS:
            put(role, turns(role))
            fetch(role, made)
            put(role, turns(role))

    blocks = GROUPS * rows // LANES
    state = {role: ([], [], set(), set()) for role in ("end", "middle")}
    results = {"end": [], "middle": []}
    packs = [code % 16 for code in ORDER if 0 <= code < 16]
    pending = {"end": {}, "middle": {}}

    def start(u, slot, role):
        roles = ("end", "middle") if role == "all" else (role,)
        key = sending(u, slot)
        before = {pending[r].get(key) for r in roles}
        assert len(before) == 1
        for old in before:
            if old is not None:
                send(*old).wait_send()
        send(u, slot).start()
        for r in roles:
            pending[r][key] = (u, slot)

    def finish(role):
        for u, slot in pending[role].values():
            send(u, slot).wait_send()
        made, given = state[role][0], results[role]
        for turn in range(len(made) - 2, len(made)):
            fin_copy(made[turn], turn).wait_send()
        for turn in range(len(given) - RESULTS, len(given)):
            result(*given[turn], turn).wait()

    def relay(u, slot, place, out):
        @pl.when(middle)
        def _():
            arrived(u, slot)
            add(rec[u][0], place, rec[u][slot])
            start(u, out, "middle")

    def phase(p, u):
        g, h, path = UNITS[u]
        d1, d2 = [d for d in path if d != "Z"]
        me1, me2 = me[d1], me[d2]
        at_z = path.index("Z")
        if p in (0, 8):
            place = packs.index(u)
            target = packed(u)

            def keep(where, value):
                target[where] = value

            if p == 0 and place >= PACKS:
                before = packs[place - PACKS]
                for slot in (0, 7) if before in SPLIT else (0,):
                    send(before, slot).wait_send()
                    for r in ("end", "middle"):
                        del pending[r][sending(before, slot)]
            gather(u, 1 - core, keep, *head(u, p == 8))
            start(u, 7 if p == 8 else 0, "all")
            return
        if p in (1, 7):
            arrived(u, 0 if p == 1 else 7)
            both = rec[u][0]

            def total(where, value):
                both[where] = both[where] + value

            gather(u, core, total, *head(u, p == 7))
            if p == 7:
                return
        if at_z == 2:
            if p == 1:
                start(u, 1, "all")
            elif p == 2:
                arrived(u, 1)
                add(rec[u][0], (me1,), rec[u][1])
                start(u, 2, "all")
            elif p == 3:
                arrived(u, 2)
                add(rec[u][0], (me1, me2), rec[u][2])

                @pl.when(end)
                def _():
                    start(u, 3, "end")
                    if h == 1:
                        start(u, 5, "end")
            elif p == 4:
                relay(u, 3, (me1, me2, far), 4)
            elif p == 5 and h == 0:
                relay(u, 4, (me1, me2, near), 6)
            elif p == 5:
                @pl.when(middle)
                def _():
                    arrived(u, 5)
                    arrived(u, 4)
                    final(u, (me1, me2, near), (5, 4), "middle")
            elif h == 0:
                @pl.when(end)
                def _():
                    arrived(u, 6)
                    final(u, (me1, me2, near), (6,), "end")
        elif at_z == 1:
            if p == 1:
                start(u, 1, "all")
            elif p == 2:
                arrived(u, 1)
                add(rec[u][0], (me1,), rec[u][1])

                @pl.when(end)
                def _():
                    start(u, 3, "end")
            elif p == 3:
                relay(u, 3, (me1, far), 4)
            elif p == 4:
                relay(u, 4, (me1, near), 6)
            elif p == 5:
                @pl.when(end)
                def _():
                    arrived(u, 6)
                    add(rec[u][0], (me1, near), rec[u][6])
                    start(u, 2, "end")
            else:
                @pl.when(end)
                def _():
                    arrived(u, 2)
                    final(u, (me1, near, me2), (2,), "end")
        else:
            if p == 1:
                @pl.when(end)
                def _():
                    start(u, 3, "end")
            elif p == 2:
                relay(u, 3, (far,), 4)
            elif p == 3:
                relay(u, 4, (near,), 6)
            elif p == 4:
                @pl.when(end)
                def _():
                    arrived(u, 6)
                    add(rec[u][0], (near,), rec[u][6])
                    start(u, 1, "end")
            elif p == 5:
                @pl.when(end)
                def _():
                    arrived(u, 1)
                    add(rec[u][0], (near, me1), rec[u][1])
                    start(u, 2, "end")
            else:
                @pl.when(end)
                def _():
                    arrived(u, 2)
                    final(u, (near, me1, me2), (2,), "end")

    multiplied, greeting = 0, True
    for code in ORDER:
        if code == MULTIPLY:
            multiply(multiplied)
            multiplied += 1
        elif code == COUPLINGS:
            coup_load.wait()
            for i in range(nh):
                mats[i] = coup[i].T
        else:
            if greeting:
                pl.semaphore_wait(barrier, len(greeted))
                order_load.wait()
                greeting = False
            phase(code // 16, code % 16)

    @pl.when(end)
    def _():
        finish("end")

    @pl.when(middle)
    def _():
        finish("middle")


def routed(size, projectors, wavefunctions, coupling, atom_order):
    rows_here, nkb = projectors.shape[1:]
    bands = wavefunctions.shape[2]
    atoms = atom_order.shape[0]
    nh, apo = nkb // atoms, coupling.shape[0]
    tile = (GROUP * nh, LANES)
    f32 = jnp.float32
    rec = []
    for _, h, path in UNITS:
        if path[0] == "Z":
            shapes = {0: (2, 2, 2), 1: (2,), 2: (), 3: (2, 2), 4: (2, 2), 6: (2, 2)}
        elif path[1] == "Z":
            shapes = {0: (2, 2, 2), 1: (2, 2), 2: (), 3: (2,), 4: (2,), 6: (2,)}
        else:
            shapes = {0: (2, 2, 2), 1: (2, 2), 2: (2,), 3: (), 4: ()}
            shapes[6 if h == 0 else 5] = ()
        rec.append({slot: pltpu.VMEM(shape + tile, f32) for slot, shape in shapes.items()})
    out = pl.pallas_call(
        functools.partial(kernel, size, nh, apo),
        out_shape=jax.ShapeDtypeStruct((LANES // 2, apo * nh), f32),
        in_specs=[
            pl.BlockSpec(memory_space=pl.ANY),
            pl.BlockSpec(memory_space=pl.ANY),
            pl.BlockSpec(memory_space=pl.ANY),
            pl.BlockSpec(memory_space=pl.ANY),
        ],
        out_specs=pl.BlockSpec(memory_space=pl.ANY),
        scratch_shapes=[
            pltpu.SMEM((atoms,), jnp.int32),
            pltpu.VMEM((LANES // 2, apo * nh), f32),
            pltpu.VMEM((2, apo * nh // 2, LANES), f32),
            pltpu.VMEM((nh, apo, nh), f32),
            pltpu.VMEM((size["Z"], nkb, LANES), f32),
            pltpu.VMEM((nkb // STRIP, 2 * rows_here, STRIP), projectors.dtype),
            pltpu.VMEM((2 * rows_here, bands), wavefunctions.dtype),
            pltpu.VMEM((nh, nh, apo), f32),
            pltpu.VMEM((PACKS, 2, 2, 2) + tile, f32),
            rec,
            pltpu.SemaphoreType.DMA((nkb // STRIP,)),
            pltpu.SemaphoreType.DMA((6,)),
            pltpu.SemaphoreType.DMA((len(UNITS) + PACKS + len(SPLIT) + GROUPS,)),
            pltpu.SemaphoreType.DMA((RECEIVES,)),
            pltpu.SemaphoreType.DMA((2,)),
            pltpu.SemaphoreType.DMA((GROUPS,)),
            pltpu.SemaphoreType.DMA((RESULTS,)),
        ],
        compiler_params=pltpu.CompilerParams(
            collective_id=0, has_side_effects=True, vmem_limit_bytes=67_043_328
        ),
    )(
        atom_order, projectors.reshape(2 * rows_here, nkb), wavefunctions.reshape(2 * rows_here, bands),
        jnp.transpose(coupling, (1, 2, 0)),
    )
    return out.T


def solution(mesh):
    gr, gc = mesh.shape["gr"], mesh.shape["gc"]
    wide = max(d for d in range(1, math.isqrt(gc) + 1) if gc % d == 0)
    size = {"A": wide, "B": gc // wide, "Z": gr // 2}

    def shards(projectors, wavefunctions, coupling, atom_order):
        fits = (
            gr % 2 == 0
            and size == {"A": 2, "B": 2, "Z": 4}
            and wavefunctions.shape[2] == size["Z"] * LANES
            and coupling.shape[0] == 2 * GROUP * GROUPS
            and coupling.shape[0] == LANES
            and projectors.shape[2] == sum(len(b) for b in BATCHES) // 2 * STRIP
        )
        if fits:
            return routed(size, projectors, wavefunctions, coupling, atom_order)
        return plain(projectors, wavefunctions, coupling, atom_order)

    return jax.shard_map(
        shards,
        mesh=mesh,
        in_specs=(
            P(None, ("gr", "gc"), None),
            P(None, ("gr", "gc"), None),
            P("gc", None, None),
            P(),
        ),
        out_specs=P("gc", "gr"),
        check_vma=False,
    )
```

```python
import functools
import math

import jax
import jax.numpy as jnp
from jax import lax
from jax.experimental import pallas as pl
from jax.experimental.pallas import tpu as pltpu
from jax.sharding import PartitionSpec as P

MESH = pl.DeviceIdType.MESH
GROUP = 8
GROUPS = 8
LANES = 128
STRIP = 1152
BATCHES = ((0, 1), (2, 3), (4, 5), (6, 7), (0, 1, 2, 3), (4, 5, 6, 7))
FIRST_PASS = 4
PACKS = 4
RESULTS = 4
MULTIPLY, COUPLINGS = -1, -2

UNITS = (
    (0, 0, "ZAB"), (1, 0, "ABZ"), (2, 0, "BAZ"), (3, 0, "ZBA"),
    (4, 0, "ABZ"), (5, 0, "ZAB"), (6, 0, "ZBA"), (7, 0, "ZBA"),
    (0, 1, "BAZ"), (1, 1, "ABZ"), (2, 1, "BAZ"), (3, 1, "ABZ"),
    (4, 1, "BAZ"), (5, 1, "ABZ"), (6, 1, "BAZ"), (7, 1, "ABZ"),
)
SPLIT = (0, 1, 2)
ORDER = (
    -1, -1, -1, -1, 1, 2, 0, -1, 129, 17, 3, 128, 130, 18, 16, -1, 19, 15, 114, 112, 8, 31, 12, 24, 14, 28, 7, 30,
    23, 34, -2, 11, 32, 27, 47, 35, 6, 22, 4, 40, 48, 20, 50, 10, 39, 26, 113, 13, 44, 51, 29, 33, 5, 66, 21, 63, 9,
    56, 38, 25, 55, 42, 37, 54, 36, 72, 53, 49, 46, 43, 65, 60, 45, 76, 52, 71, 59, 79, 68, 41, 82, 67, 75, 61, 64,
    84, 77, 58, 88, 70, 81, 74, 57, 62, 69, 83, 100, 87, 95, 93, 73, 98, 80, 97, 92, 85, 86, 91, 109, 96, 78, 103,
    107, 90, 89, 99, 101, 94, 111, 108, 106, 102, 105, 110, 104,
)


def receiving():
    found, count = {}, 0
    for u, (_, h, path) in enumerate(UNITS):
        at_z = path.index("Z")
        if at_z == 0:
            sets = [(0,), (3, 6), (4, 1), (2,)]
        elif at_z == 1:
            sets = [(0,), (1,), (3, 6), (4, 2)]
        else:
            sets = [(0,), (1,), (2,), (3, 6), (4,)] + ([(5,)] if h == 1 else [])
        if u in SPLIT:
            sets.append((7,))
        for slots in sets:
            found.update({(u, slot): count for slot in slots})
            count += 1
    return found, count


RECEIVING, RECEIVES = receiving()


def plain(projectors, wavefunctions, coupling, atom_order):
    rows_here, nkb = projectors.shape[1:]
    bands = wavefunctions.shape[2]
    atoms = atom_order.shape[0]
    nh = nkb // atoms
    shaped = projectors.reshape(2, rows_here, atoms, nh)
    waves = wavefunctions.reshape(2 * rows_here, bands)
    columns = jnp.take(shaped, atom_order, axis=2).reshape(2 * rows_here, nkb)
    term = lax.dot_general(columns, waves, (((0,), (0,)), ((), ())), preferred_element_type=jnp.float32)
    partial_rows = lax.psum_scatter(2.0 * term, "gc", scatter_dimension=0, tiled=True)
    becp = lax.psum_scatter(partial_rows, "gr", scatter_dimension=1, tiled=True)
    local_atoms = coupling.shape[0]
    becp = becp.reshape(local_atoms, nh, becp.shape[1])
    coupled = jnp.einsum("kij,kjb->kib", coupling, becp, precision=lax.Precision.HIGHEST)
    return coupled.reshape(local_atoms * nh, becp.shape[2])


def kernel(
    size, nh, apo, order_in, proj_ref, wave_in, coup_in, out_ref, order_ref, turned, fin, mats, nat, strip, wave, coup,
    oth, rec, strip_sem, load_sem, send_sem, recv_sem, fin_send, fin_recv, out_sem,
):
    gr, gc = lax.axis_index("gr"), lax.axis_index("gc")
    core, z = lax.rem(gr, 2), gr // 2
    me = {"A": gc // size["B"], "B": lax.rem(gc, size["B"])}
    half = apo // 2
    rows = GROUP * nh
    side = z // 2
    near, far = side, 1 - side
    way = 1 - 2 * side
    end = (z == 0) | (z == size["Z"] - 1)
    middle = jnp.logical_not(end)

    def at(a, b, zz):
        return {"gr": zz * 2 + core, "gc": a * size["B"] + b}

    partner = {"gr": gr + 1 - 2 * core, "gc": gc}
    other = {"A": at(1 - me["A"], me["B"], z), "B": at(me["A"], 1 - me["B"], z)}
    inward = at(me["A"], me["B"], z + way)
    outward = at(me["A"], me["B"], lax.rem(z - way + size["Z"], size["Z"]))

    strips = proj_ref.shape[1] // STRIP

    def load(number):
        return pltpu.make_async_copy(proj_ref.at[:, pl.ds(number * STRIP, STRIP)], strip.at[number], strip_sem.at[number])

    wave_loads = [
        pltpu.make_async_copy(wave_in.at[:, pl.ds(zz * LANES, LANES)], wave.at[:, pl.ds(i * LANES, LANES)], load_sem.at[i])
        for i, zz in enumerate((0, 3, 1, 2))
    ]
    coup_load = pltpu.make_async_copy(coup_in, coup, load_sem.at[4])
    order_load = pltpu.make_async_copy(order_in, order_ref, load_sem.at[5])
    wave_loads[0].start()
    wave_loads[1].start()
    for number in range(strips):
        load(number).start()
    order_load.start()
    wave_loads[2].start()
    wave_loads[3].start()
    coup_load.start()

    greeted = [partner, other["A"], other["B"], inward, outward]
    barrier = pltpu.get_barrier_semaphore()
    for device in greeted:
        pl.semaphore_signal(barrier, inc=1, device_id=device, device_id_type=MESH)

    def multiply(batch):
        h = int(batch >= FIRST_PASS)
        if batch in (0, FIRST_PASS):
            wave_loads[2 * h].wait()
            wave_loads[2 * h + 1].wait()
        if h == 0:
            for number in BATCHES[batch]:
                load(number).wait()
        for number in BATCHES[batch]:
            term = lax.dot_general(
                strip[number], wave[:, 2 * h * LANES:2 * (h + 1) * LANES],
                (((0,), (0,)), ((), ())), preferred_element_type=jnp.float32,
            )
            for i in range(2):
                nat[2 * h + i, pl.ds(number * STRIP, STRIP), :] = term[:, i * LANES:(i + 1) * LANES]

    def first_of(u):
        path = UNITS[u][2]
        return far if path[0] == "Z" else 1 - me[path[0]]

    def gather(u, which, store, fixed=None):
        g, h, path = UNITS[u]

        def body(t, carry):
            of = {}
            if fixed is None or path[0] == "Z":
                of = {"A": t // size["B"], "B": lax.rem(t, size["B"])}
            else:
                of = {path[0]: fixed, "B" if path[0] == "A" else "A": t}
            owner = of["A"] * size["B"] + of["B"]
            for i in range(GROUP):
                row = order_ref[owner * apo + which * half + g * GROUP + i] * nh
                for zi in ((0, 1) if fixed is None or path[0] != "Z" else (fixed,)):
                    of["Z"] = zi
                    where = tuple(of[d] for d in path) + (pl.ds(i * nh, nh), slice(None))
                    store(where, nat[2 * h + zi, pl.ds(row, nh), :])
            return carry

        lax.fori_loop(0, size["A"] * size["B"] if fixed is None or path[0] == "Z" else 2, body, 0)

    def add(dst, prefix, src):
        rest = src.shape[:-2]
        if len(rest) == 2:
            def body(t, carry):
                where = (t // rest[1], lax.rem(t, rest[1]))
                dst[tuple(prefix) + where] = dst[tuple(prefix) + where] + src[where]
                return carry

            lax.fori_loop(0, math.prod(rest), body, 0)
        elif rest:
            for t in range(rest[0]):
                dst[tuple(prefix) + (t,)] = dst[tuple(prefix) + (t,)] + src[t]
        else:
            dst[tuple(prefix)] = dst[tuple(prefix)] + src[...]

    def copy(u, slot, src, dst, device):
        return pltpu.make_async_remote_copy(
            src_ref=src, dst_ref=dst, send_sem=send_sem.at[sending(u, slot)], recv_sem=recv_sem.at[RECEIVING[u, slot]],
            device_id=device, device_id_type=MESH,
        )

    def sending(u, slot):
        if slot == 0:
            return len(UNITS) + packs.index(u) % PACKS
        if slot == 7:
            return len(UNITS) + PACKS + SPLIT.index(u)
        if slot == 5:
            return len(UNITS) + PACKS + len(SPLIT) + UNITS[u][0]
        return u

    def packed(u):
        return oth.at[packs.index(u) % PACKS]

    def head(u, rest):
        if u not in SPLIT:
            return ()
        return (1 - first_of(u) if rest else first_of(u),)

    def buffers(u, slot):
        if slot in (0, 7):
            return rec[u][0].at[head(u, slot == 7)] if u in SPLIT else rec[u][0]
        return rec[u][slot]

    def send(u, slot):
        g, h, path = UNITS[u]
        d1, d2 = [d for d in path if d != "Z"]
        me1, me2 = me[d1], me[d2]
        to = buffers(u, slot)
        if slot in (0, 7):
            return copy(u, slot, packed(u).at[head(u, slot == 7)] if u in SPLIT else packed(u), to, partner)
        at_z = path.index("Z")
        place = (me1, me2)[:at_z]
        src = {3: place + (far,), 4: place + (far,), 5: place + (near,), 6: place + (near,)}
        if at_z == 0:
            src[1], src[2] = (near, 1 - me1), (near, me1, 1 - me2)
        elif at_z == 1:
            src[1], src[2] = (1 - me1,), (me1, near, 1 - me2)
        else:
            src[1], src[2] = (1 - me1,), (me1, 1 - me2)
        device = {1: other[d1], 2: other[d2], 3: inward, 4: inward, 5: inward, 6: outward}[slot]
        return copy(u, slot, rec[u][0].at[src[slot]], to, device)

    def arrived(u, slot):
        to = buffers(u, slot)
        copy(u, slot, to, to, partner).wait_recv()

    def fin_copy(g, turn):
        part = fin.at[core, pl.ds(g * rows, rows)]
        return pltpu.make_async_remote_copy(
            src_ref=part, dst_ref=part, send_sem=fin_send.at[turn % 2], recv_sem=fin_recv.at[g],
            device_id=partner, device_id_type=MESH,
        )

    def ready(groups):
        return {t for t in range(blocks) if all(g in groups for g in range(t * LANES // rows, (t * LANES + LANES - 1) // rows + 1))}

    def result(t, mine, turn):
        which = core if mine else 1 - core
        columns = pl.ds(pl.multiple_of((which * blocks + t) * LANES, LANES), LANES)
        return pltpu.make_async_copy(turned.at[:, columns], out_ref.at[:, columns], out_sem.at[turn % RESULTS])

    def turn(t, mine):
        which = core if mine else 1 - core
        block = fin[which, pl.ds(t * LANES, LANES), :].T
        own = LANES // 2
        to = pl.ds(pl.multiple_of((which * blocks + t) * LANES, LANES), LANES)
        turned[:, to] = jnp.where(core == 0, block[:own], block[own:])

    def come(g):
        part = fin.at[1 - core, pl.ds(g * rows, rows)]
        pltpu.make_async_remote_copy(
            src_ref=part, dst_ref=part, send_sem=fin_send.at[0], recv_sem=fin_recv.at[g],
            device_id=partner, device_id_type=MESH,
        ).wait_recv()

    def fetch(role, groups):
        came = state[role][1]
        for g in groups:
            if g not in came:
                come(g)
                came.append(g)

    def turns(role):
        made, came, mine, theirs = state[role]
        found = [(t, True) for t in sorted(ready(made) - mine)] + [(t, False) for t in sorted(ready(came) - theirs)]
        for t, own in found:
            turn(t, own)
            (mine if own else theirs).add(t)
        return found

    def put(role, found):
        given = results[role]
        for t, own in found:
            if len(given) >= RESULTS:
                result(*given[-RESULTS], len(given) - RESULTS).wait()
            result(t, own, len(given)).start()
            given.append((t, own))

    def final(u, own, others, role):
        g = UNITS[u][0]
        made = state[role][0]
        fetch(role, made[:-1])
        found = turns(role)
        for i in range(GROUP):
            here = (pl.ds(i * nh, nh), slice(None))
            becp = rec[u][0][own + here]
            for slot in others:
                becp = becp + rec[u][slot][here]
            fin[core, pl.ds((g * GROUP + i) * nh, nh), :] = jnp.dot(
                mats[:, pl.ds(core * half + g * GROUP + i, 1), :].reshape(nh, nh), 2.0 * becp,
                precision=lax.Precision.HIGHEST, preferred_element_type=jnp.float32,
            )
        if len(made) >= 2:
            fin_copy(made[-2], len(made) - 2).wait_send()
        fin_copy(g, len(made)).start()
        made.append(g)
        put(role, found)
        if len(made) == GROUPS:
            put(role, turns(role))
            fetch(role, made)
            put(role, turns(role))

    blocks = GROUPS * rows // LANES
    state = {role: ([], [], set(), set()) for role in ("end", "middle")}
    results = {"end": [], "middle": []}
    packs = [code % 16 for code in ORDER if 0 <= code < 16]
    pending = {"end": {}, "middle": {}}

    def start(u, slot, role):
        roles = ("end", "middle") if role == "all" else (role,)
        key = sending(u, slot)
        before = {pending[r].get(key) for r in roles}
        assert len(before) == 1
        for old in before:
            if old is not None:
                send(*old).wait_send()
        send(u, slot).start()
        for r in roles:
            pending[r][key] = (u, slot)

    def finish(role):
        for u, slot in pending[role].values():
            send(u, slot).wait_send()
        made, given = state[role][0], results[role]
        for turn in range(len(made) - 2, len(made)):
            fin_copy(made[turn], turn).wait_send()
        for turn in range(len(given) - RESULTS, len(given)):
            result(*given[turn], turn).wait()

    def relay(u, slot, place, out):
        @pl.when(middle)
        def _():
            arrived(u, slot)
            add(rec[u][0], place, rec[u][slot])
            start(u, out, "middle")

    def phase(p, u):
        g, h, path = UNITS[u]
        d1, d2 = [d for d in path if d != "Z"]
        me1, me2 = me[d1], me[d2]
        at_z = path.index("Z")
        if p in (0, 8):
            place = packs.index(u)
            target = packed(u)

            def keep(where, value):
                target[where] = value

            if p == 0 and place >= PACKS:
                before = packs[place - PACKS]
                for slot in (0, 7) if before in SPLIT else (0,):
                    send(before, slot).wait_send()
                    for r in ("end", "middle"):
                        del pending[r][sending(before, slot)]
            gather(u, 1 - core, keep, *head(u, p == 8))
            start(u, 7 if p == 8 else 0, "all")
            return
        if p in (1, 7):
            arrived(u, 0 if p == 1 else 7)
            both = rec[u][0]

            def total(where, value):
                both[where] = both[where] + value

            gather(u, core, total, *head(u, p == 7))
            if p == 7:
                return
        if at_z == 2:
            if p == 1:
                start(u, 1, "all")
            elif p == 2:
                arrived(u, 1)
                add(rec[u][0], (me1,), rec[u][1])
                start(u, 2, "all")
            elif p == 3:
                arrived(u, 2)
                add(rec[u][0], (me1, me2), rec[u][2])

                @pl.when(end)
                def _():
                    start(u, 3, "end")
                    if h == 1:
                        start(u, 5, "end")
            elif p == 4:
                relay(u, 3, (me1, me2, far), 4)
            elif p == 5 and h == 0:
                relay(u, 4, (me1, me2, near), 6)
            elif p == 5:
                @pl.when(middle)
                def _():
                    arrived(u, 5)
                    arrived(u, 4)
                    final(u, (me1, me2, near), (5, 4), "middle")
            elif h == 0:
                @pl.when(end)
                def _():
                    arrived(u, 6)
                    final(u, (me1, me2, near), (6,), "end")
        elif at_z == 1:
            if p == 1:
                start(u, 1, "all")
            elif p == 2:
                arrived(u, 1)
                add(rec[u][0], (me1,), rec[u][1])

                @pl.when(end)
                def _():
                    start(u, 3, "end")
            elif p == 3:
                relay(u, 3, (me1, far), 4)
            elif p == 4:
                relay(u, 4, (me1, near), 6)
            elif p == 5:
                @pl.when(end)
                def _():
                    arrived(u, 6)
                    add(rec[u][0], (me1, near), rec[u][6])
                    start(u, 2, "end")
            else:
                @pl.when(end)
                def _():
                    arrived(u, 2)
                    final(u, (me1, near, me2), (2,), "end")
        else:
            if p == 1:
                @pl.when(end)
                def _():
                    start(u, 3, "end")
            elif p == 2:
                relay(u, 3, (far,), 4)
            elif p == 3:
                relay(u, 4, (near,), 6)
            elif p == 4:
                @pl.when(end)
                def _():
                    arrived(u, 6)
                    add(rec[u][0], (near,), rec[u][6])
                    start(u, 1, "end")
            elif p == 5:
                @pl.when(end)
                def _():
                    arrived(u, 1)
                    add(rec[u][0], (near, me1), rec[u][1])
                    start(u, 2, "end")
            else:
                @pl.when(end)
                def _():
                    arrived(u, 2)
                    final(u, (near, me1, me2), (2,), "end")

    multiplied, greeting = 0, True
    for code in ORDER:
        if code == MULTIPLY:
            multiply(multiplied)
            multiplied += 1
        elif code == COUPLINGS:
            coup_load.wait()
            for i in range(nh):
                mats[i] = coup[i].T
        else:
            if greeting:
                pl.semaphore_wait(barrier, len(greeted))
                order_load.wait()
                greeting = False
            phase(code // 16, code % 16)

    @pl.when(end)
    def _():
        finish("end")

    @pl.when(middle)
    def _():
        finish("middle")


def routed(size, projectors, wavefunctions, coupling, atom_order):
    rows_here, nkb = projectors.shape[1:]
    bands = wavefunctions.shape[2]
    atoms = atom_order.shape[0]
    nh, apo = nkb // atoms, coupling.shape[0]
    tile = (GROUP * nh, LANES)
    f32 = jnp.float32
    rec = []
    for _, h, path in UNITS:
        if path[0] == "Z":
            shapes = {0: (2, 2, 2), 1: (2,), 2: (), 3: (2, 2), 4: (2, 2), 6: (2, 2)}
        elif path[1] == "Z":
            shapes = {0: (2, 2, 2), 1: (2, 2), 2: (), 3: (2,), 4: (2,), 6: (2,)}
        else:
            shapes = {0: (2, 2, 2), 1: (2, 2), 2: (2,), 3: (), 4: ()}
            shapes[6 if h == 0 else 5] = ()
        rec.append({slot: pltpu.VMEM(shape + tile, f32) for slot, shape in shapes.items()})
    out = pl.pallas_call(
        functools.partial(kernel, size, nh, apo),
        out_shape=jax.ShapeDtypeStruct((LANES // 2, apo * nh), f32),
        in_specs=[
            pl.BlockSpec(memory_space=pl.ANY),
            pl.BlockSpec(memory_space=pl.ANY),
            pl.BlockSpec(memory_space=pl.ANY),
            pl.BlockSpec(memory_space=pl.ANY),
        ],
        out_specs=pl.BlockSpec(memory_space=pl.ANY),
        scratch_shapes=[
            pltpu.SMEM((atoms,), jnp.int32),
            pltpu.VMEM((LANES // 2, apo * nh), f32),
            pltpu.VMEM((2, apo * nh // 2, LANES), f32),
            pltpu.VMEM((nh, apo, nh), f32),
            pltpu.VMEM((size["Z"], nkb, LANES), f32),
            pltpu.VMEM((nkb // STRIP, 2 * rows_here, STRIP), projectors.dtype),
            pltpu.VMEM((2 * rows_here, bands), wavefunctions.dtype),
            pltpu.VMEM((nh, nh, apo), f32),
            pltpu.VMEM((PACKS, 2, 2, 2) + tile, f32),
            rec,
            pltpu.SemaphoreType.DMA((nkb // STRIP,)),
            pltpu.SemaphoreType.DMA((6,)),
            pltpu.SemaphoreType.DMA((len(UNITS) + PACKS + len(SPLIT) + GROUPS,)),
            pltpu.SemaphoreType.DMA((RECEIVES,)),
            pltpu.SemaphoreType.DMA((2,)),
            pltpu.SemaphoreType.DMA((GROUPS,)),
            pltpu.SemaphoreType.DMA((RESULTS,)),
        ],
        compiler_params=pltpu.CompilerParams(
            collective_id=0, has_side_effects=True, vmem_limit_bytes=67_043_328
        ),
    )(
        atom_order, projectors.reshape(2 * rows_here, nkb), wavefunctions.reshape(2 * rows_here, bands),
        jnp.transpose(coupling, (1, 2, 0)),
    )
    return out.T


def solution(mesh):
    gr, gc = mesh.shape["gr"], mesh.shape["gc"]
    wide = max(d for d in range(1, math.isqrt(gc) + 1) if gc % d == 0)
    size = {"A": wide, "B": gc // wide, "Z": gr // 2}

    def shards(projectors, wavefunctions, coupling, atom_order):
        fits = (
            gr % 2 == 0
            and size == {"A": 2, "B": 2, "Z": 4}
            and wavefunctions.shape[2] == size["Z"] * LANES
            and coupling.shape[0] == 2 * GROUP * GROUPS
            and coupling.shape[0] == LANES
            and projectors.shape[2] == sum(len(b) for b in BATCHES) // 2 * STRIP
        )
        if fits:
            return routed(size, projectors, wavefunctions, coupling, atom_order)
        return plain(projectors, wavefunctions, coupling, atom_order)

    return jax.shard_map(
        shards,
        mesh=mesh,
        in_specs=(
            P(None, ("gr", "gc"), None),
            P(None, ("gr", "gc"), None),
            P("gc", None, None),
            P(),
        ),
        out_specs=P("gc", "gr"),
        check_vma=False,
    )
```
